32 devices in a mesh: rows: 32 (over z, y, x, core).
Axes of the slice: x: 2, y: 2, z: 4, core: 2. Of those that a mesh axis runs over, the one named last changes fastest.
Arguments:
- points: float32 [8, 131072], P(None, 'rows'), may hold values from -6 to 6
- scales: float32 [8], replicated, may hold values from 1 to 3
- noise_var: float32 [131072], P('rows'), may hold values from 0.05 to 0.5
- pivots: int32 [8, 16], replicated, may hold values from 0 to 131071, as said below
Outputs:
- factor: float32 [128, 131072], P(None, 'rows')
- residual_diag: float32 [131072], P('rows')
- mean_residual: float32 [8], replicated
The draws below stay inside these ranges and needn't reach their ends.
Inputs may be any that keep to these rules, and one draw needn't show every extreme that they name: `pivots`: all 128 entries are distinct point indices.
All inputs are finite; a program needn't handle non-finite values.
Results may differ from the reference program's by a relative error of at most 0.00014.
Values sent between devices are 32-bit elements; how exact they have to be, the bound alone decides.
A program may use at most 64 MiB of HBM per device.

```python
import math
import jax
import jax.numpy as jnp
from jax import lax

DIM = 8
BS = 16
BLOCKS = 8
NPTS = 131072


def draw_pivots(key, part):
    chosen = jax.random.permutation(key, NPTS)[:BLOCKS * BS]
    return chosen.reshape((BLOCKS, BS)).astype(jnp.int32)


def block_scale(own_key, extent, split, low, top_value):
    level = 1.0
    for dim, parts in split:
        draws = jax.random.uniform(jax.random.fold_in(jax.random.fold_in(own_key, 6), dim), (parts,), jnp.float32, low / len(split), top_value / len(split))
        level = level * jnp.repeat(jnp.exp(draws), extent[dim] // parts).reshape((-1,) + (1,) * (len(extent) - 1 - dim))
    return level


def centred(own_key, dims, width, reach, split=(), kind=jnp.bfloat16):
    array = jax.random.normal(own_key, dims, jnp.float32) * width
    if len(split) > 0:
        array = block_scale(own_key, dims, split, -0.22, 0.18) * array
    return jnp.clip(array, min=-reach, max=reach).astype(kind)


def setup_inputs(seed: int = 0) -> dict:
    keys = jax.random.split(jax.random.key(seed), 5)
    points = centred(keys[0], (DIM, NPTS), 1.0, 6.0, ((1, 32),), jnp.float32)
    scales = jnp.clip(jnp.exp(jax.random.uniform(keys[1], (DIM,), jnp.float32, math.log(1.0), math.log(3.0))), 1.0, 3.0)
    noise_var = jnp.clip(jnp.exp(math.log(0.5) - 2.3025851 * jax.random.uniform(keys[2], (NPTS,), jnp.float32) ** block_scale(keys[2], (NPTS,), ((0, 32),), -0.2, 0.2)), 0.05, 0.5)
    pivots = draw_pivots(jax.random.fold_in(keys[4], 71), 0)
    return dict(points=points, scales=scales, noise_var=noise_var, pivots=pivots)


def kernel(first_coords, second_coords):
    summed = jnp.zeros((first_coords.shape[1], second_coords.shape[1]), jnp.float32)
    for axis_pos in range(first_coords.shape[0]):
        differ = first_coords[axis_pos][:, None] - second_coords[axis_pos][None, :]
        summed = summed + differ * differ
    return jnp.exp(-0.5 * summed)

def reference(points, scales, noise_var, pivots):
    scaled = points / scales[:, None]
    point_count = points.shape[1]
    point_ids = jnp.arange(point_count, dtype=jnp.int32)
    residual_diag = 1.0 + noise_var
    done_rows = []
    averages = []
    for block_idx in range(BLOCKS):
        wanted = pivots[block_idx]
        pivot_coords = jnp.take(scaled, wanted, axis=1)
        columns = kernel(pivot_coords, scaled) + jnp.where(point_ids[None, :] == wanted[:, None], noise_var[None, :], 0.0)
        for earlier in done_rows:
            picked = jnp.take(earlier, wanted, axis=1)
            columns = columns - jnp.dot(picked.T.astype(jnp.float32), earlier.astype(jnp.float32), precision=lax.Precision.HIGHEST, preferred_element_type=jnp.float32)
        pivot_block = jnp.take(columns, wanted, axis=1)
        chol_block = jnp.linalg.cholesky(pivot_block)
        new_rows = lax.linalg.triangular_solve(chol_block, columns, left_side=True, lower=True)
        done_rows.append(new_rows)
        residual_diag = residual_diag - jnp.sum(new_rows * new_rows, axis=0)
        averages.append(jnp.sum(residual_diag) / point_count)
    return (jnp.concatenate(done_rows, axis=0), residual_diag, jnp.stack(averages))
```

```python
import functools

import jax
import jax.numpy as jnp
from jax import lax
from jax.experimental import pallas as pl
from jax.experimental.pallas import tpu as pltpu
from jax.sharding import PartitionSpec as P

LANES = 128
SUB = 8
F32 = jnp.float32
BF16 = jnp.bfloat16


def split3(x):
    high = x.astype(BF16).astype(F32)
    rest = x - high
    mid = rest.astype(BF16).astype(F32)
    low = (rest - mid).astype(BF16).astype(F32)
    return high, mid, low


def load_points(dim, points, scale, noise, packed):
    packed[0:dim, :] = points[...] / scale
    packed[dim : 2 * dim, :] = jnp.broadcast_to(noise[...], (dim, noise.shape[1]))


def scale_column(dim, scales):
    axis_pos = lax.broadcasted_iota(jnp.int32, (dim, 1), 0)
    scale = jnp.ones((dim, 1), F32)
    for d in range(dim):
        scale = jnp.where(axis_pos == d, scales[d], scale)
    return scale


def gather_own(offset, pivot_row, points, noise_tiles):
    dim, width = points.shape
    ranks = pivot_row.shape[1]
    wanted = jnp.broadcast_to(pivot_row - offset, (SUB, ranks))
    lane = jnp.bitwise_and(wanted, LANES - 1)
    tile = jnp.right_shift(wanted, 7)
    own = jnp.zeros((dim, ranks), F32)
    for t in range(width // LANES):
        part = points[:, t * LANES : (t + 1) * LANES]
        own = jnp.where(tile == t, jnp.take_along_axis(part, lane, axis=1), own)
    row = lax.broadcasted_iota(jnp.int32, (SUB, ranks), 0)
    own_noise = jnp.zeros((SUB, ranks), F32)
    for t in range(0, width // LANES, SUB):
        part = noise_tiles[t : t + SUB, :]
        own_noise = jnp.where(
            tile == row + t, jnp.take_along_axis(part, lane, axis=1), own_noise
        )
    return own, jnp.sum(own_noise, axis=0, keepdims=True)


def partners(n, group, me):
    low, high = lax.rem(me, group), me - lax.rem(me, group)
    near = [high + lax.rem(low + k, group) for k in range(1, group)]
    far = [lax.rem(me + k * group, n) for k in range(1, n // group)]
    return near, far


def exchange(devices, slots, send_sem, recv_sem):
    for k, device in enumerate(devices):
        pltpu.make_async_remote_copy(
            src_ref=slots.at[0],
            dst_ref=slots.at[k + 1],
            send_sem=send_sem,
            recv_sem=recv_sem,
            device_id=(device,),
            device_id_type=pl.DeviceIdType.MESH,
        ).start()


def all_of(devices, slots, send_sem, recv_sem):
    rest = slots.at[pl.ds(1, len(devices))]
    return pltpu.make_async_remote_copy(
        src_ref=rest,
        dst_ref=rest,
        send_sem=send_sem,
        recv_sem=recv_sem,
        device_id=(devices[0],),
        device_id_type=pl.DeviceIdType.MESH,
    )


def total_of(slots):
    total = slots[0]
    for k in range(1, slots.shape[0]):
        total = total + slots[k]
    return total


def pivot_covariance(dim, coords):
    ranks = coords.shape[1]
    across = coords.T
    total = jnp.zeros((ranks, ranks), F32)
    for d in range(dim):
        differ = across[:, d : d + 1] - coords[d : d + 1, :]
        total = total + differ * differ
    row = lax.broadcasted_iota(jnp.int32, (ranks, ranks), 0)
    col = lax.broadcasted_iota(jnp.int32, (ranks, ranks), 1)
    cov = jnp.exp(-0.5 * total) + jnp.where(row == col, coords[dim : dim + 1, :], 0.0)
    return cov, (row == col).astype(F32)


def eliminate(left, right, first_lane):
    shape = left[0].shape
    a = [
        [
            jnp.broadcast_to(left[i][:, first_lane + j : first_lane + j + 1], shape)
            for j in range(i + 1)
        ]
        for i in range(SUB)
    ]
    inverse = []
    for k in range(SUB):
        r = lax.rsqrt(a[k][k])
        inverse.append(r)
        left[k] = left[k] * r
        right[k] = right[k] * r
        for i in range(k + 1, SUB):
            a[i][k] = a[i][k] * r
        for i in range(k + 1, SUB):
            for j in range(k + 1, i + 1):
                a[i][j] = a[i][j] - a[i][k] * a[j][k]
            left[i] = left[i] - a[i][k] * left[k]
            right[i] = right[i] - a[i][k] * right[k]
    return a, inverse


def spread(rows):
    return [jnp.broadcast_to(rows[i : i + 1], rows.shape) for i in range(SUB)]


def gathered(rows):
    return jnp.concatenate([rows[i][i : i + 1] for i in range(SUB)], axis=0)


def factor_rows(ranks, state):
    step = 2 * SUB
    for lo in range(0, ranks, step):
        mid, hi = lo + SUB, lo + step
        left = spread(state[lo:mid, 0:ranks])
        right = spread(state[lo:mid, ranks : 2 * ranks])
        low_left = state[mid:hi, 0:ranks]
        low_right = state[mid:hi, ranks : 2 * ranks]
        start = [
            jnp.broadcast_to(low_left[:, lo + k : lo + k + 1], (SUB, ranks))
            for k in range(SUB)
        ]
        mult, inverse = eliminate(left, right, lo)
        cols = []
        for k in range(SUB):
            col = start[k]
            for j in range(k):
                col = col - cols[j] * mult[k][j]
            cols.append(col * inverse[k])
        for k in range(SUB):
            low_left = low_left - cols[k] * left[k]
            low_right = low_right - cols[k] * right[k]
        next_left, next_right = spread(low_left), spread(low_right)
        eliminate(next_left, next_right, mid)
        new_left = jnp.concatenate([gathered(left), gathered(next_left)], axis=0)
        new_right = jnp.concatenate([gathered(right), gathered(next_right)], axis=0)
        state[lo:hi, ranks : 2 * ranks] = new_right
        if hi < ranks:
            new = jnp.concatenate([new_left, new_right], axis=1)
            h, m, l = split3(new)
            lh, lm, ll = (x[:, 0:ranks] for x in (h, m, l))
            one = jnp.concatenate([lh, lh, lh, lm, lm, ll], axis=0).T[hi:ranks].astype(BF16)
            two = jnp.concatenate([h, m, l, h, m, h], axis=0).astype(BF16)
            state[hi:ranks, :] = state[hi:ranks, :] - jnp.dot(
                one, two, preferred_element_type=F32
            )


def pivot_side(dim, coords, centre):
    y = coords[0:dim, :] - centre
    yh, ym, yl = split3(y)
    nh, nm, nl = split3(-0.5 * jnp.sum(y * y, axis=0, keepdims=True))
    ones = jnp.ones_like(nh)
    tail = [ones, ones, ones, nh, nm, nl, jnp.zeros((dim - 6, y.shape[1]), F32)]
    return jnp.concatenate([yh, yh, ym, ym, yh, yl] + tail, axis=0).T.astype(BF16)


def point_side(dim, x):
    xh, xm, xl = split3(x)
    nh, nm, nl = split3(-0.5 * jnp.sum(x * x, axis=0, keepdims=True))
    ones = jnp.ones_like(nh)
    tail = [nh, nm, nl, ones, ones, ones, jnp.zeros((dim - 6, x.shape[1]), F32)]
    return jnp.concatenate([xh, xm, xh, xm, xl, xh] + tail, axis=0).astype(BF16)


def body_kernel(
    n, group, blocks, chunk,
    points, scales, noise, noise_tiles, pivots,
    factor, residual, averages,
    packed, near_slots, far_slots, state, after, near_sums, far_sums,
    send_sem, recv_sem,
):
    dim, width = points.shape
    ranks = factor.shape[0]
    per_block = ranks // blocks
    me = lax.axis_index("rows")
    offset = me * width
    near, far = partners(n, group, me)

    barrier = pltpu.get_barrier_semaphore()
    for device in near + far:
        pl.semaphore_signal(
            barrier, inc=1, device_id=(device,), device_id_type=pl.DeviceIdType.MESH
        )
    scale = scale_column(dim, scales)
    pivot_row = jnp.concatenate([pivots[b : b + 1, :] for b in range(blocks)], axis=1)
    own, own_noise = gather_own(offset, pivot_row, points, noise_tiles)
    own = own / scale
    for d in range(dim):
        near_slots[0, d] = own[d : d + 1]
    near_slots[0, dim] = own_noise
    pl.semaphore_wait(barrier, len(near) + len(far))
    first = (near, near_slots, send_sem.at[0], recv_sem.at[0])
    second = (far, far_slots, send_sem.at[1], recv_sem.at[1])
    exchange(*first)
    load_points(dim, points, scale, noise, packed)
    all_of(*first).wait_recv()
    far_slots[0] = total_of(near_slots)
    exchange(*second)
    all_of(*second).wait_recv()
    coords = total_of(far_slots)
    coords = jnp.concatenate([coords[d] for d in range(dim + 1)], axis=0)

    cov, eye = pivot_covariance(dim, coords)
    state[:, 0:ranks] = cov
    state[:, ranks : 2 * ranks] = eye
    factor_rows(ranks, state)
    row = lax.broadcasted_iota(jnp.int32, (ranks, ranks), 0)
    col = lax.broadcasted_iota(jnp.int32, (ranks, ranks), 1)
    solve = jnp.where(row >= col, state[:, ranks : 2 * ranks], 0.0)

    centre = jnp.sum(coords[0:dim, :], axis=1, keepdims=True) / ranks
    side = pivot_side(dim, coords, centre)
    local_row = (pivot_row - offset).astype(F32)
    local_col = jnp.broadcast_to(local_row, (SUB, ranks)).T[:, 0:1].astype(jnp.int32)
    for c in range(width // chunk):
        at = slice(c * chunk, (c + 1) * chunk)
        x = packed[0:dim, at] - centre
        cross = jnp.exp(jnp.dot(side, point_side(dim, x), preferred_element_type=F32))
        noise_row = packed[dim : dim + 1, at]
        ids = lax.broadcasted_iota(jnp.int32, (ranks, chunk), 1) + c * chunk
        cross = cross + jnp.where(ids == local_col, noise_row, 0.0)
        rows = jnp.dot(
            solve, cross, precision=lax.Precision.HIGHEST, preferred_element_type=F32
        )
        factor[:, at] = rows
        left = 1.0 + noise_row
        for b in range(blocks):
            part = rows[b * per_block : (b + 1) * per_block]
            left = left - jnp.sum(part * part, axis=0, keepdims=True)
            after[b : b + 1, at] = left
        residual[at] = left[0]

    total = jnp.zeros((blocks, LANES), F32)
    for c in range(width // LANES):
        total = total + after[:, c * LANES : (c + 1) * LANES]
    total = jnp.sum(total, axis=1, keepdims=True)
    row = lax.broadcasted_iota(jnp.int32, (blocks, LANES), 0)
    col = lax.broadcasted_iota(jnp.int32, (blocks, LANES), 1)
    near_sums[0] = jnp.sum(jnp.where(row == col, total, 0.0), axis=0, keepdims=True)
    third = (near, near_sums, send_sem.at[2], recv_sem.at[2])
    fourth = (far, far_sums, send_sem.at[3], recv_sem.at[3])
    exchange(*third)
    all_of(*third).wait_recv()
    far_sums[0] = total_of(near_sums)
    exchange(*fourth)
    all_of(*fourth).wait_recv()
    total = total_of(far_sums)
    for step in (first, second, third, fourth):
        all_of(*step).wait_send()
    averages[...] = total[0, 0:blocks] / (width * n)


def store_kernel(factor, residual, averages, to_factor, to_residual, to_averages, sem):
    copies = [
        pltpu.make_async_copy(source, target, sem.at[i])
        for i, (source, target) in enumerate(
            [(factor, to_factor), (residual, to_residual), (averages, to_averages)]
        )
    ]
    for copy in copies:
        copy.start()
    for copy in copies:
        copy.wait()


def body(n, points, scales, noise_var, pivots):
    dim, width = points.shape
    blocks, per_block = pivots.shape
    ranks = blocks * per_block
    chunk = 512
    group = 1
    while group * group < n:
        group *= 2
    vmem = pl.BlockSpec(memory_space=pltpu.VMEM)
    factor, residual, averages = pl.pallas_call(
        functools.partial(body_kernel, n, group, blocks, chunk),
        name="whole",
        out_shape=(
            pltpu.VMEM((ranks, width), F32),
            pltpu.VMEM((width,), F32),
            pltpu.VMEM((blocks,), F32),
        ),
        in_specs=[
            vmem, pl.BlockSpec(memory_space=pltpu.SMEM), vmem, vmem, vmem,
        ],
        out_specs=(vmem, vmem, vmem),
        scratch_shapes=[
            pltpu.VMEM((2 * dim, width), F32),
            pltpu.VMEM((group, dim + 1, 1, ranks), F32),
            pltpu.VMEM((n // group, dim + 1, 1, ranks), F32),
            pltpu.VMEM((ranks, 2 * ranks), F32),
            pltpu.VMEM((blocks, width), F32),
            pltpu.VMEM((group, 1, LANES), F32),
            pltpu.VMEM((n // group, 1, LANES), F32),
            pltpu.SemaphoreType.DMA((4,)),
            pltpu.SemaphoreType.DMA((4,)),
        ],
        compiler_params=pltpu.CompilerParams(collective_id=0, has_side_effects=True),
    )(points, scales, noise_var.reshape(1, -1), noise_var.reshape(-1, LANES), pivots)
    anywhere = pl.BlockSpec(memory_space=pl.ANY)
    return pl.pallas_call(
        store_kernel,
        name="store",
        out_shape=(
            jax.ShapeDtypeStruct((ranks, width), F32),
            jax.ShapeDtypeStruct((width,), F32),
            jax.ShapeDtypeStruct((blocks,), F32),
        ),
        in_specs=[vmem] * 3,
        out_specs=(anywhere,) * 3,
        scratch_shapes=[pltpu.SemaphoreType.DMA((3,))],
    )(*(pltpu.with_memory_space_constraint(x, pltpu.VMEM) for x in (factor, residual, averages)))


def solution(mesh):
    in_specs = (P(None, "rows"), P(), P("rows"), P())
    out_specs = (P(None, "rows"), P("rows"), P())
    return jax.shard_map(
        functools.partial(body, mesh.shape["rows"]),
        mesh=mesh, in_specs=in_specs, out_specs=out_specs, check_vma=False,
    )
```

```python
import functools

import jax
import jax.numpy as jnp
from jax import lax
from jax.experimental import pallas as pl
from jax.experimental.pallas import tpu as pltpu
from jax.sharding import PartitionSpec as P

LANES = 128
SUB = 8
F32 = jnp.float32
BF16 = jnp.bfloat16


def split3(x):
    high = x.astype(BF16).astype(F32)
    rest = x - high
    mid = rest.astype(BF16).astype(F32)
    low = (rest - mid).astype(BF16).astype(F32)
    return high, mid, low


def scale_column(dim, scales):
    axis_pos = lax.broadcasted_iota(jnp.int32, (dim, 1), 0)
    scale = jnp.ones((dim, 1), F32)
    for d in range(dim):
        scale = jnp.where(axis_pos == d, scales[d], scale)
    return scale


def gather_own(offset, pivot_row, points, noise_tiles):
    dim, width = points.shape
    ranks = pivot_row.shape[1]
    wanted = jnp.broadcast_to(pivot_row - offset, (SUB, ranks))
    lane = jnp.bitwise_and(wanted, LANES - 1)
    tile = jnp.right_shift(wanted, 7)
    own = jnp.zeros((dim, ranks), F32)
    for t in range(width // LANES):
        part = points[:, t * LANES : (t + 1) * LANES]
        own = jnp.where(tile == t, jnp.take_along_axis(part, lane, axis=1), own)
    row = lax.broadcasted_iota(jnp.int32, (SUB, ranks), 0)
    own_noise = jnp.zeros((SUB, ranks), F32)
    for t in range(0, width // LANES, SUB):
        part = noise_tiles[t : t + SUB, :]
        own_noise = jnp.where(
            tile == row + t, jnp.take_along_axis(part, lane, axis=1), own_noise
        )
    return own, jnp.sum(own_noise, axis=0, keepdims=True)


def pivot_covariance(dim, coords):
    ranks = coords.shape[1]
    across = coords.T
    total = jnp.zeros((ranks, ranks), F32)
    for d in range(dim):
        differ = across[:, d : d + 1] - coords[d : d + 1, :]
        total = total + differ * differ
    row = lax.broadcasted_iota(jnp.int32, (ranks, ranks), 0)
    col = lax.broadcasted_iota(jnp.int32, (ranks, ranks), 1)
    cov = jnp.exp(-0.5 * total) + jnp.where(row == col, coords[dim : dim + 1, :], 0.0)
    return cov, (row == col).astype(F32)


def eliminate(left, right, first_lane):
    shape = left[0].shape
    a = [
        [
            jnp.broadcast_to(left[i][:, first_lane + j : first_lane + j + 1], shape)
            for j in range(i + 1)
        ]
        for i in range(SUB)
    ]
    inverse = []
    for k in range(SUB):
        r = lax.rsqrt(a[k][k])
        inverse.append(r)
        left[k] = left[k] * r
        right[k] = right[k] * r
        for i in range(k + 1, SUB):
            a[i][k] = a[i][k] * r
        for i in range(k + 1, SUB):
            for j in range(k + 1, i + 1):
                a[i][j] = a[i][j] - a[i][k] * a[j][k]
            left[i] = left[i] - a[i][k] * left[k]
            right[i] = right[i] - a[i][k] * right[k]
    return a, inverse


def spread(rows):
    return [jnp.broadcast_to(rows[i : i + 1], rows.shape) for i in range(SUB)]


def gathered(rows):
    return jnp.concatenate([rows[i][i : i + 1] for i in range(SUB)], axis=0)


def factor_rows(ranks, state, between):
    step = 2 * SUB
    for lo in range(0, ranks, step):
        mid, hi = lo + SUB, lo + step
        left = spread(state[lo:mid, 0:ranks])
        right = spread(state[lo:mid, ranks : 2 * ranks])
        low_left = state[mid:hi, 0:ranks]
        low_right = state[mid:hi, ranks : 2 * ranks]
        start = [
            jnp.broadcast_to(low_left[:, lo + k : lo + k + 1], (SUB, ranks))
            for k in range(SUB)
        ]
        mult, inverse = eliminate(left, right, lo)
        cols = []
        for k in range(SUB):
            col = start[k]
            for j in range(k):
                col = col - cols[j] * mult[k][j]
            cols.append(col * inverse[k])
        for k in range(SUB):
            low_left = low_left - cols[k] * left[k]
            low_right = low_right - cols[k] * right[k]
        next_left, next_right = spread(low_left), spread(low_right)
        eliminate(next_left, next_right, mid)
        new_left = jnp.concatenate([gathered(left), gathered(next_left)], axis=0)
        new_right = jnp.concatenate([gathered(right), gathered(next_right)], axis=0)
        state[lo:hi, ranks : 2 * ranks] = new_right
        if hi < ranks:
            new = jnp.concatenate([new_left, new_right], axis=1)
            h, m, l = split3(new)
            lh, lm, ll = (x[:, 0:ranks] for x in (h, m, l))
            one = jnp.concatenate([lh, lh, lh, lm, lm, ll], axis=0).T[hi:ranks].astype(BF16)
            two = jnp.concatenate([h, m, l, h, m, h], axis=0).astype(BF16)
            state[hi:ranks, :] = state[hi:ranks, :] - jnp.dot(
                one, two, preferred_element_type=F32
            )
        between(lo // step)


def pivot_side(dim, coords, centre):
    y = coords[0:dim, :] - centre
    yh, ym, yl = split3(y)
    nh, nm, nl = split3(-0.5 * jnp.sum(y * y, axis=0, keepdims=True))
    ones = jnp.ones_like(nh)
    tail = [ones, ones, ones, nh, nm, nl, jnp.zeros((2 * dim - 6, y.shape[1]), F32)]
    return jnp.concatenate([yh, yh, ym, ym, yh, yl] + tail, axis=0).T.astype(BF16)


def point_side(dim, x):
    xh, xm, xl = split3(x)
    nh, nm, nl = split3(-0.5 * jnp.sum(x * x, axis=0, keepdims=True))
    ones = jnp.ones_like(nh)
    tail = [nh, nm, nl, ones, ones, ones, jnp.zeros((2 * dim - 6, x.shape[1]), F32)]
    return jnp.concatenate([xh, xm, xh, xm, xl, xh] + tail, axis=0).astype(BF16)


def send(slots, k, device, send_sem, recv_sem):
    pltpu.make_async_remote_copy(
        src_ref=slots.at[0],
        dst_ref=slots.at[k],
        send_sem=send_sem,
        recv_sem=recv_sem,
        device_id=(device,),
        device_id_type=pl.DeviceIdType.MESH,
    ).start()


def all_of(slots, device, send_sem, recv_sem):
    rest = slots.at[pl.ds(1, slots.shape[0] - 1)]
    return pltpu.make_async_remote_copy(
        src_ref=rest,
        dst_ref=rest,
        send_sem=send_sem,
        recv_sem=recv_sem,
        device_id=(device,),
        device_id_type=pl.DeviceIdType.MESH,
    )


def total_of(slots):
    parts = [slots[k] for k in range(slots.shape[0])]
    while len(parts) > 1:
        parts = [a + b for a, b in zip(parts[::2], parts[1::2])] + (
            parts[-1:] if len(parts) % 2 else []
        )
    return parts[0]


def signal(sem, device):
    pl.semaphore_signal(
        sem, inc=1, device_id=(device,), device_id_type=pl.DeviceIdType.MESH
    )


def body_kernel(
    n, group, blocks, chunk,
    from_points, from_scales, from_noise, from_tiles, from_pivots,
    factor, residual, averages,
    points, scales, noise, noise_tiles, pivots,
    near_slots, far_slots, sum_slots, state, sides, pieces,
    load_sem, send_sem, recv_sem, ready_sem,
):
    dim, width = points.shape
    ranks = factor.shape[0]
    per_block = ranks // blocks
    me = lax.axis_index("rows")
    offset = me * width
    far_count = n // group
    low = lax.rem(me, group)
    level = (me - low) // group
    near = [me - low + lax.rem(low + k, group) for k in range(1, group)]
    far = [lax.rem(me + k * group, n) for k in range(1, far_count)]

    loads = [
        pltpu.make_async_copy(source, target, load_sem.at[i])
        for i, (source, target) in enumerate(
            [
                (from_points, points), (from_scales, scales), (from_noise, noise),
                (from_tiles, noise_tiles), (from_pivots, pivots),
            ]
        )
    ]
    for load in loads:
        load.start()
    barrier = pltpu.get_barrier_semaphore()
    for device in near:
        signal(barrier, device)
    for k in range(1, far_count):

        @pl.when(level + k < far_count)
        def _():
            signal(barrier, me + k * group)

    for load in loads:
        load.wait()
    scale = scale_column(dim, scales)
    pivot_row = jnp.concatenate([pivots[b : b + 1, :] for b in range(blocks)], axis=1)
    own, own_noise = gather_own(offset, pivot_row, points, noise_tiles)
    own = own / scale
    for d in range(dim):
        near_slots[0, d] = own[d : d + 1]
    near_slots[0, dim] = own_noise
    pl.semaphore_wait(barrier, group - 1 + level)
    for k, device in enumerate(near):
        send(near_slots, k + 1, device, send_sem.at[0], recv_sem.at[0])
    for k in range(1, far_count):

        @pl.when(level >= k)
        def _():
            signal(ready_sem, me - k * group)

    centre = jnp.sum(points[...], axis=1, keepdims=True) / (width * scale)
    base = jnp.zeros((SUB, LANES), F32)
    for t in range(0, width // LANES, SUB):
        base = base + (1.0 + noise_tiles[t : t + SUB, :])
    base = jnp.sum(jnp.sum(base, axis=1, keepdims=True), axis=0, keepdims=True)
    for c in range(width // chunk):
        at = slice(c * chunk, (c + 1) * chunk)
        sides[:, at] = point_side(dim, points[:, at] / scale - centre)

    all_of(near_slots, near[0], send_sem.at[0], recv_sem.at[0]).wait_recv()
    far_slots[0] = total_of(near_slots)

    @pl.when(level < far_count - 1)
    def _():
        pl.semaphore_wait(ready_sem, far_count - 1 - level)

    for k, device in enumerate(far):
        send(far_slots, k + 1, device, send_sem.at[1], recv_sem.at[1])
    all_of(far_slots, far[0], send_sem.at[1], recv_sem.at[1]).wait_recv()
    coords = total_of(far_slots)
    coords = jnp.concatenate([coords[d] for d in range(dim + 1)], axis=0)

    cov, eye = pivot_covariance(dim, coords)
    state[:, 0:ranks] = cov
    state[:, ranks : 2 * ranks] = eye
    side = pivot_side(dim, coords, centre)
    local_row = (pivot_row - offset).astype(F32)
    local_col = jnp.broadcast_to(local_row, (SUB, ranks)).T[:, 0:1].astype(jnp.int32)

    def cross_chunk(c):
        if c >= width // chunk:
            return
        at = slice(c * chunk, (c + 1) * chunk)
        cross = jnp.exp(jnp.dot(side, sides[:, at], preferred_element_type=F32))
        ids = lax.broadcasted_iota(jnp.int32, (ranks, chunk), 1) + c * chunk
        cross = cross + jnp.where(ids == local_col, noise[:, at], 0.0)
        high = cross.astype(BF16)
        rest = cross - high.astype(F32)
        mid = rest.astype(BF16)
        pieces[0:ranks, at] = high
        pieces[ranks : 2 * ranks, at] = mid
        pieces[2 * ranks : 3 * ranks, at] = (rest - mid.astype(F32)).astype(BF16)

    rounds = ranks // (2 * SUB)
    each = -(-(width // chunk) // rounds)

    def between(r):
        for c in range(r * each, (r + 1) * each):
            cross_chunk(c)

    factor_rows(ranks, state, between)
    row = lax.broadcasted_iota(jnp.int32, (ranks, ranks), 0)
    col = lax.broadcasted_iota(jnp.int32, (ranks, ranks), 1)
    solve = jnp.where(row >= col, state[:, ranks : 2 * ranks], 0.0)
    sh, sm, sl = (x.astype(BF16) for x in split3(solve))
    lefts = [jnp.concatenate(pair, axis=1) for pair in [(sh, sh), (sm, sm), (sl, sh)]]

    totals = [jnp.zeros((SUB, LANES), F32) for _ in range(blocks)]
    for c in range(width // chunk):
        at = slice(c * chunk, (c + 1) * chunk)
        one = pieces[0 : 2 * ranks, at]
        two = jnp.concatenate(
            [pieces[0:ranks, at], pieces[2 * ranks : 3 * ranks, at]], axis=0
        )
        rows = (
            jnp.dot(lefts[0], one, preferred_element_type=F32)
            + jnp.dot(lefts[1], one, preferred_element_type=F32)
            + jnp.dot(lefts[2], two, preferred_element_type=F32)
        )
        factor[:, at] = rows
        square = rows * rows
        explained = jnp.zeros((SUB, chunk), F32)
        for b in range(blocks):
            part = jnp.zeros((SUB, chunk), F32)
            for i in range(b * per_block, (b + 1) * per_block, SUB):
                part = part + square[i : i + SUB]
            explained = explained + part
            for j in range(0, chunk, LANES):
                totals[b] = totals[b] + part[:, j : j + LANES]
        left = 1.0 + noise[:, at] - jnp.sum(explained, axis=0, keepdims=True)
        residual[at] = left[0]

    total = jnp.concatenate([jnp.sum(x, axis=0, keepdims=True) for x in totals], axis=0)
    total = jnp.sum(total, axis=1, keepdims=True)
    row = lax.broadcasted_iota(jnp.int32, (blocks, LANES), 0)
    col = lax.broadcasted_iota(jnp.int32, (blocks, LANES), 1)
    done = jnp.sum(jnp.where(row <= col, total, 0.0), axis=0, keepdims=True)
    sum_slots[0] = base - done

    def send_sum(k, carry):
        send(sum_slots, k, lax.rem(me + k, n), send_sem.at[2], recv_sem.at[2])
        return carry

    lax.fori_loop(1, n, send_sum, 0)
    last = all_of(sum_slots, near[0], send_sem.at[2], recv_sem.at[2])
    all_of(near_slots, near[0], send_sem.at[0], recv_sem.at[0]).wait_send()
    all_of(far_slots, far[0], send_sem.at[1], recv_sem.at[1]).wait_send()
    last.wait_send()
    last.wait_recv()
    averages[...] = total_of(sum_slots)[0, 0:blocks] / (width * n)


def store_kernel(factor, residual, averages, to_factor, to_residual, to_averages, sem):
    copies = [
        pltpu.make_async_copy(source, target, sem.at[i])
        for i, (source, target) in enumerate(
            [(factor, to_factor), (residual, to_residual), (averages, to_averages)]
        )
    ]
    for copy in copies:
        copy.start()
    for copy in copies:
        copy.wait()


def body(n, points, scales, noise_var, pivots):
    dim, width = points.shape
    blocks, per_block = pivots.shape
    ranks = blocks * per_block
    chunk = 512
    group = 1
    while group * group < n:
        group *= 2
    vmem = pl.BlockSpec(memory_space=pltpu.VMEM)
    anywhere = pl.BlockSpec(memory_space=pl.ANY)
    factor, residual, averages = pl.pallas_call(
        functools.partial(body_kernel, n, group, blocks, chunk),
        name="whole",
        out_shape=(
            pltpu.VMEM((ranks, width), F32),
            pltpu.VMEM((width,), F32),
            pltpu.VMEM((blocks,), F32),
        ),
        in_specs=[anywhere] * 5,
        out_specs=(vmem, vmem, vmem),
        scratch_shapes=[
            pltpu.VMEM((dim, width), F32),
            pltpu.SMEM((dim,), F32),
            pltpu.VMEM((1, width), F32),
            pltpu.VMEM((width // LANES, LANES), F32),
            pltpu.VMEM(pivots.shape, jnp.int32),
            pltpu.VMEM((group, dim + 1, 1, ranks), F32),
            pltpu.VMEM((n // group, dim + 1, 1, ranks), F32),
            pltpu.VMEM((n, 1, LANES), F32),
            pltpu.VMEM((ranks, 2 * ranks), F32),
            pltpu.VMEM((8 * dim, width), BF16),
            pltpu.VMEM((3 * ranks, width), BF16),
            pltpu.SemaphoreType.DMA((5,)),
            pltpu.SemaphoreType.DMA((3,)),
            pltpu.SemaphoreType.DMA((3,)),
            pltpu.SemaphoreType.REGULAR,
        ],
        compiler_params=pltpu.CompilerParams(collective_id=0, has_side_effects=True),
    )(points, scales, noise_var.reshape(1, -1), noise_var.reshape(-1, LANES), pivots)
    return pl.pallas_call(
        store_kernel,
        name="store",
        out_shape=(
            jax.ShapeDtypeStruct((ranks, width), F32),
            jax.ShapeDtypeStruct((width,), F32),
            jax.ShapeDtypeStruct((blocks,), F32),
        ),
        in_specs=[vmem] * 3,
        out_specs=(anywhere,) * 3,
        scratch_shapes=[pltpu.SemaphoreType.DMA((3,))],
    )(*(pltpu.with_memory_space_constraint(x, pltpu.VMEM) for x in (factor, residual, averages)))


def solution(mesh):
    in_specs = (P(None, "rows"), P(), P("rows"), P())
    out_specs = (P(None, "rows"), P("rows"), P())
    return jax.shard_map(
        functools.partial(body, mesh.shape["rows"]),
        mesh=mesh, in_specs=in_specs, out_specs=out_specs, check_vma=False,
    )
```

```python
import functools
import math

import jax
import jax.numpy as jnp
from jax import lax
from jax.experimental import pallas as pl
from jax.experimental.pallas import tpu as pltpu
from jax.sharding import PartitionSpec as P

LANES = 128
SUB = 8
F32 = jnp.float32
BF16 = jnp.bfloat16
LOG2E = math.log2(math.e)


def split3(x):
    high = x.astype(BF16).astype(F32)
    rest = x - high
    mid = rest.astype(BF16).astype(F32)
    low = (rest - mid).astype(BF16).astype(F32)
    return high, mid, low


def scale_column(dim, scales):
    axis_pos = lax.broadcasted_iota(jnp.int32, (dim, 1), 0)
    scale = jnp.ones((dim, 1), F32)
    for d in range(dim):
        scale = jnp.where(axis_pos == d, scales[d], scale)
    return scale


def gather_own(offset, pivot_row, points, noise_tiles):
    dim, width = points.shape
    ranks = pivot_row.shape[1]
    wanted = jnp.broadcast_to(pivot_row - offset, (SUB, ranks))
    lane = jnp.bitwise_and(wanted, LANES - 1)
    tile = jnp.right_shift(wanted, 7)
    own = jnp.zeros((dim, ranks), F32)
    for t in range(width // LANES):
        part = points[:, t * LANES : (t + 1) * LANES]
        own = jnp.where(tile == t, jnp.take_along_axis(part, lane, axis=1), own)
    row = lax.broadcasted_iota(jnp.int32, (SUB, ranks), 0)
    own_noise = jnp.zeros((SUB, ranks), F32)
    for t in range(0, width // LANES, SUB):
        part = noise_tiles[t : t + SUB, :]
        own_noise = jnp.where(
            tile == row + t, jnp.take_along_axis(part, lane, axis=1), own_noise
        )
    return own, jnp.sum(own_noise, axis=0, keepdims=True)


def pivot_covariance(dim, coords):
    ranks = coords.shape[1]
    across = coords.T
    total = jnp.zeros((ranks, ranks), F32)
    for d in range(dim):
        differ = across[:, d : d + 1] - coords[d : d + 1, :]
        total = total + differ * differ
    row = lax.broadcasted_iota(jnp.int32, (ranks, ranks), 0)
    col = lax.broadcasted_iota(jnp.int32, (ranks, ranks), 1)
    return jnp.exp(-0.5 * total) + jnp.where(row == col, coords[dim : dim + 1, :], 0.0)


def over_rows(x, i):
    return jnp.broadcast_to(x[i % SUB : i % SUB + 1], x.shape)


def over_lanes(x, j):
    return jnp.broadcast_to(x[:, j : j + 1], x.shape)


def eliminate(rows, cols, low_rows, low_cols):
    size = SUB * len(rows)
    diag = over_rows(cols[0][0], 0)
    done = []
    for k in range(size):
        own = k // SUB
        r = lax.rsqrt(diag)
        if k + 1 < size:
            after = (k + 1) // SUB
            step = over_rows(cols[k][after], k + 1) * r
            diag = over_rows(cols[k + 1][after], k + 1) - step * step
        unit = over_rows(rows[own], k) * r
        done.append(unit)
        col = [cols[k][v] * r if v >= own else None for v in range(len(rows))]
        low_col = [x * r for x in low_cols[k]]
        for j in range(k + 1, size):
            m = over_rows(col[j // SUB], j)
            for v in range(j // SUB, len(rows)):
                cols[j][v] = cols[j][v] - col[v] * m
            for v in range(len(low_rows)):
                low_cols[j][v] = low_cols[j][v] - low_col[v] * m
        for v in range((k + 1) // SUB, len(rows)):
            rows[v] = rows[v] - col[v] * unit
        for v in range(len(low_rows)):
            low_rows[v] = low_rows[v] - low_col[v] * unit
    return [
        jnp.concatenate([done[i][i % SUB : i % SUB + 1] for i in range(v, v + SUB)], axis=0)
        for v in range(0, size, SUB)
    ]


def outer_update(done, hi):
    h, m, l = split3(jnp.concatenate(done, axis=0))
    one = jnp.concatenate([h, h, h, m, m, l], axis=0).T[hi:].astype(BF16)
    two = jnp.concatenate([h, m, l, h, m, h], axis=0).astype(BF16)
    return jnp.dot(one, two, preferred_element_type=F32)


def factor_rows(ranks, state, between):
    size = 2 * SUB
    row = lax.broadcasted_iota(jnp.int32, (SUB, ranks), 0)
    col = lax.broadcasted_iota(jnp.int32, (SUB, ranks), 1)

    def columns(rows, at):
        return [
            [over_lanes(x, j) if at + v * SUB + SUB > j else None for v, x in enumerate(rows)]
            for j in range(at, at + size)
        ]

    def opened(rows, first, at):
        inside = jnp.logical_and(col >= at, col < at + size)
        return [
            jnp.where(inside, jnp.where(row + (first + v * SUB) == col, 1.0, 0.0), x)
            for v, x in enumerate(rows)
        ]

    for lo in range(0, ranks, 2 * size):
        mid, hi = lo + size, lo + 2 * size
        rows = [state[i : i + SUB, :] for i in range(lo, mid, SUB)]
        low_rows = [state[i : i + SUB, :] for i in range(mid, hi, SUB)]
        cols = columns(rows, lo)
        low_cols = [[over_lanes(x, j) for x in low_rows] for j in range(lo, mid)]
        rows, low_rows = opened(rows, lo, lo), opened(low_rows, mid, lo)
        first = eliminate(rows, cols, low_rows, low_cols)
        first = [jnp.where(jnp.logical_and(col >= mid, col < hi), 0.0, x) for x in first]
        cols = columns(low_rows, mid)
        low_rows = opened(low_rows, mid, mid)
        second = eliminate(low_rows, cols, [], [[] for _ in range(size)])
        for v, x in enumerate(first + second):
            state[lo + v * SUB : lo + v * SUB + SUB, :] = x
        if hi < ranks:
            update = outer_update(first, hi) + outer_update(second, hi)
            wide = lax.broadcasted_iota(jnp.int32, update.shape, 1)
            kept = jnp.where(jnp.logical_and(wide >= lo, wide < hi), 0.0, state[hi:, :])
            state[hi:, :] = kept - update
        between(lo // (2 * size))


def pivot_side(dim, coords, centre):
    y = coords[0:dim, :] - centre
    yh, ym, yl = split3(LOG2E * y)
    nh, nm, nl = split3((-0.5 * LOG2E) * jnp.sum(y * y, axis=0, keepdims=True))
    ones = jnp.ones_like(nh)
    tail = [ones, ones, ones, nh, nm, nl, jnp.zeros((2 * dim - 6, y.shape[1]), F32)]
    return jnp.concatenate([yh, yh, ym, ym, yh, yl] + tail, axis=0).T.astype(BF16)


def point_side(dim, x):
    xh, xm, xl = split3(x)
    nh, nm, nl = split3((-0.5 * LOG2E) * jnp.sum(x * x, axis=0, keepdims=True))
    ones = jnp.ones_like(nh)
    tail = [nh, nm, nl, ones, ones, ones, jnp.zeros((2 * dim - 6, x.shape[1]), F32)]
    return jnp.concatenate([xh, xm, xh, xm, xl, xh] + tail, axis=0).astype(BF16)


def send(slots, k, device, send_sem, recv_sem):
    pltpu.make_async_remote_copy(
        src_ref=slots.at[0],
        dst_ref=slots.at[k],
        send_sem=send_sem,
        recv_sem=recv_sem,
        device_id=(device,),
        device_id_type=pl.DeviceIdType.MESH,
    ).start()


def all_of(slots, device, send_sem, recv_sem):
    rest = slots.at[pl.ds(1, slots.shape[0] - 1)]
    return pltpu.make_async_remote_copy(
        src_ref=rest,
        dst_ref=rest,
        send_sem=send_sem,
        recv_sem=recv_sem,
        device_id=(device,),
        device_id_type=pl.DeviceIdType.MESH,
    )


def total_of(slots):
    parts = [slots[k] for k in range(slots.shape[0])]
    while len(parts) > 1:
        parts = [a + b for a, b in zip(parts[::2], parts[1::2])] + (
            parts[-1:] if len(parts) % 2 else []
        )
    return parts[0]


def signal(sem, device):
    pl.semaphore_signal(
        sem, inc=1, device_id=(device,), device_id_type=pl.DeviceIdType.MESH
    )


def body_kernel(
    n, group, blocks, chunk,
    from_points, from_scales, from_noise, from_tiles, from_pivots,
    factor, residual, averages,
    points, scales, noise, noise_tiles, pivots,
    near_slots, far_slots, sum_slots, state, sides, pieces,
    load_sem, send_sem, recv_sem, ready_sem,
):
    dim, width = points.shape
    ranks = factor.shape[0]
    per_block = ranks // blocks
    me = lax.axis_index("rows")
    offset = me * width
    far_count = n // group
    low = lax.rem(me, group)
    level = (me - low) // group
    near = [me - low + lax.rem(low + k, group) for k in range(1, group)]
    far = [lax.rem(me + k * group, n) for k in range(1, far_count)]

    loads = [
        pltpu.make_async_copy(source, target, load_sem.at[i])
        for i, (source, target) in enumerate(
            [
                (from_points, points), (from_scales, scales), (from_noise, noise),
                (from_tiles, noise_tiles), (from_pivots, pivots),
            ]
        )
    ]
    for load in loads:
        load.start()
    barrier = pltpu.get_barrier_semaphore()
    for device in near:
        signal(barrier, device)
    for k in range(1, far_count):

        @pl.when(level + k < far_count)
        def _():
            signal(barrier, me + k * group)

    for load in loads:
        load.wait()
    scale = scale_column(dim, scales)
    pivot_row = jnp.concatenate([pivots[b : b + 1, :] for b in range(blocks)], axis=1)
    own, own_noise = gather_own(offset, pivot_row, points, noise_tiles)
    own = own / scale
    for d in range(dim):
        near_slots[0, d] = own[d : d + 1]
    near_slots[0, dim] = own_noise
    pl.semaphore_wait(barrier, group - 1 + level)
    for k, device in enumerate(near):
        send(near_slots, k + 1, device, send_sem.at[0], recv_sem.at[0])
    for k in range(1, far_count):

        @pl.when(level >= k)
        def _():
            signal(ready_sem, me - k * group)

    centre = jnp.sum(points[...], axis=1, keepdims=True) / (width * scale)
    base = jnp.zeros((SUB, LANES), F32)
    for t in range(0, width // LANES, SUB):
        base = base + (1.0 + noise_tiles[t : t + SUB, :])
    base = jnp.sum(jnp.sum(base, axis=1, keepdims=True), axis=0, keepdims=True)
    for c in range(width // chunk):
        at = slice(c * chunk, (c + 1) * chunk)
        sides[:, at] = point_side(dim, points[:, at] / scale - centre)

    all_of(near_slots, near[0], send_sem.at[0], recv_sem.at[0]).wait_recv()
    far_slots[0] = total_of(near_slots)

    @pl.when(level < far_count - 1)
    def _():
        pl.semaphore_wait(ready_sem, far_count - 1 - level)

    for k, device in enumerate(far):
        send(far_slots, k + 1, device, send_sem.at[1], recv_sem.at[1])
    all_of(far_slots, far[0], send_sem.at[1], recv_sem.at[1]).wait_recv()
    coords = total_of(far_slots)
    coords = jnp.concatenate([coords[d] for d in range(dim + 1)], axis=0)

    state[...] = pivot_covariance(dim, coords)
    side = pivot_side(dim, coords, centre)
    local_row = (pivot_row - offset).astype(F32)
    local_col = jnp.broadcast_to(local_row, (SUB, ranks)).T[:, 0:1].astype(jnp.int32)

    def cross_chunk(c):
        if c >= width // chunk:
            return
        at = slice(c * chunk, (c + 1) * chunk)
        cross = jnp.exp2(jnp.dot(side, sides[:, at], preferred_element_type=F32))
        ids = lax.broadcasted_iota(jnp.int32, (ranks, chunk), 1) + c * chunk
        cross = jnp.where(ids == local_col, 1.0 + noise[:, at], cross)
        high = cross.astype(BF16)
        pieces[0:ranks, at] = high
        pieces[ranks : 2 * ranks, at] = (cross - high.astype(F32)).astype(BF16)

    rounds = ranks // (4 * SUB)
    each = -(-(width // chunk) // rounds)

    def between(r):
        for c in range(r * each, (r + 1) * each):
            cross_chunk(c)

    factor_rows(ranks, state, between)
    row = lax.broadcasted_iota(jnp.int32, (ranks, ranks), 0)
    col = lax.broadcasted_iota(jnp.int32, (ranks, ranks), 1)
    solve = jnp.where(row >= col, state[...], 0.0)
    high = solve.astype(BF16)
    lefts = [
        jnp.concatenate([x, x], axis=1)
        for x in (high, (solve - high.astype(F32)).astype(BF16))
    ]

    totals = [jnp.zeros((SUB, LANES), F32) for _ in range(blocks)]
    for c in range(width // chunk):
        at = slice(c * chunk, (c + 1) * chunk)
        one = pieces[:, at]
        rows = jnp.dot(lefts[0], one, preferred_element_type=F32) + jnp.dot(
            lefts[1], one, preferred_element_type=F32
        )
        factor[:, at] = rows
        square = rows * rows
        explained = jnp.zeros((SUB, chunk), F32)
        for b in range(blocks):
            part = jnp.zeros((SUB, chunk), F32)
            for i in range(b * per_block, (b + 1) * per_block, SUB):
                part = part + square[i : i + SUB]
            explained = explained + part
            for j in range(0, chunk, LANES):
                totals[b] = totals[b] + part[:, j : j + LANES]
        left = 1.0 + noise[:, at] - jnp.sum(explained, axis=0, keepdims=True)
        residual[at] = left[0]

    total = jnp.concatenate([jnp.sum(x, axis=0, keepdims=True) for x in totals], axis=0)
    total = jnp.sum(total, axis=1, keepdims=True)
    row = lax.broadcasted_iota(jnp.int32, (blocks, LANES), 0)
    col = lax.broadcasted_iota(jnp.int32, (blocks, LANES), 1)
    done = jnp.sum(jnp.where(row <= col, total, 0.0), axis=0, keepdims=True)
    sum_slots[0] = base - done

    def send_sum(k, carry):
        send(sum_slots, k, lax.rem(me + k, n), send_sem.at[2], recv_sem.at[2])
        return carry

    lax.fori_loop(1, n, send_sum, 0)
    last = all_of(sum_slots, near[0], send_sem.at[2], recv_sem.at[2])
    all_of(near_slots, near[0], send_sem.at[0], recv_sem.at[0]).wait_send()
    all_of(far_slots, far[0], send_sem.at[1], recv_sem.at[1]).wait_send()
    last.wait_send()
    last.wait_recv()
    averages[...] = total_of(sum_slots)[0, 0:blocks] / (width * n)


def store_kernel(factor, residual, averages, to_factor, to_residual, to_averages, sem):
    copies = [
        pltpu.make_async_copy(source, target, sem.at[i])
        for i, (source, target) in enumerate(
            [(factor, to_factor), (residual, to_residual), (averages, to_averages)]
        )
    ]
    for copy in copies:
        copy.start()
    for copy in copies:
        copy.wait()


def body(n, points, scales, noise_var, pivots):
    dim, width = points.shape
    blocks, per_block = pivots.shape
    ranks = blocks * per_block
    chunk = 512
    group = 1
    while group * group < n:
        group *= 2
    vmem = pl.BlockSpec(memory_space=pltpu.VMEM)
    anywhere = pl.BlockSpec(memory_space=pl.ANY)
    factor, residual, averages = pl.pallas_call(
        functools.partial(body_kernel, n, group, blocks, chunk),
        name="whole",
        out_shape=(
            pltpu.VMEM((ranks, width), F32),
            pltpu.VMEM((width,), F32),
            pltpu.VMEM((blocks,), F32),
        ),
        in_specs=[anywhere] * 5,
        out_specs=(vmem, vmem, vmem),
        scratch_shapes=[
            pltpu.VMEM((dim, width), F32),
            pltpu.SMEM((dim,), F32),
            pltpu.VMEM((1, width), F32),
            pltpu.VMEM((width // LANES, LANES), F32),
            pltpu.VMEM(pivots.shape, jnp.int32),
            pltpu.VMEM((group, dim + 1, 1, ranks), F32),
            pltpu.VMEM((n // group, dim + 1, 1, ranks), F32),
            pltpu.VMEM((n, 1, LANES), F32),
            pltpu.VMEM((ranks, ranks), F32),
            pltpu.VMEM((8 * dim, width), BF16),
            pltpu.VMEM((2 * ranks, width), BF16),
            pltpu.SemaphoreType.DMA((5,)),
            pltpu.SemaphoreType.DMA((3,)),
            pltpu.SemaphoreType.DMA((3,)),
            pltpu.SemaphoreType.REGULAR,
        ],
        compiler_params=pltpu.CompilerParams(collective_id=0, has_side_effects=True),
    )(points, scales, noise_var.reshape(1, -1), noise_var.reshape(-1, LANES), pivots)
    return pl.pallas_call(
        store_kernel,
        name="store",
        out_shape=(
            jax.ShapeDtypeStruct((ranks, width), F32),
            jax.ShapeDtypeStruct((width,), F32),
            jax.ShapeDtypeStruct((blocks,), F32),
        ),
        in_specs=[vmem] * 3,
        out_specs=(anywhere,) * 3,
        scratch_shapes=[pltpu.SemaphoreType.DMA((3,))],
    )(*(pltpu.with_memory_space_constraint(x, pltpu.VMEM) for x in (factor, residual, averages)))


def solution(mesh):
    in_specs = (P(None, "rows"), P(), P("rows"), P())
    out_specs = (P(None, "rows"), P("rows"), P())
    return jax.shard_map(
        functools.partial(body, mesh.shape["rows"]),
        mesh=mesh, in_specs=in_specs, out_specs=out_specs, check_vma=False,
    )
```

```python
import functools
import math

import jax
import jax.numpy as jnp
from jax import lax
from jax.experimental import pallas as pl
from jax.experimental.pallas import tpu as pltpu
from jax.sharding import PartitionSpec as P

LANES = 128
SUB = 8
F32 = jnp.float32
BF16 = jnp.bfloat16
LOG2E = math.log2(math.e)


def split3(x):
    high = x.astype(BF16).astype(F32)
    rest = x - high
    mid = rest.astype(BF16).astype(F32)
    low = (rest - mid).astype(BF16).astype(F32)
    return high, mid, low


def scale_column(dim, scales):
    axis_pos = lax.broadcasted_iota(jnp.int32, (dim, 1), 0)
    scale = jnp.ones((dim, 1), F32)
    for d in range(dim):
        scale = jnp.where(axis_pos == d, scales[d], scale)
    return scale


def gather_own(offset, pivot_row, points, noise_tiles):
    dim, width = points.shape
    ranks = pivot_row.shape[1]
    wanted = jnp.broadcast_to(pivot_row - offset, (SUB, ranks))
    lane = jnp.bitwise_and(wanted, LANES - 1)
    tile = jnp.right_shift(wanted, 7)
    own = jnp.zeros((dim, ranks), F32)
    for t in range(width // LANES):
        part = points[:, t * LANES : (t + 1) * LANES]
        own = jnp.where(tile == t, jnp.take_along_axis(part, lane, axis=1), own)
    row = lax.broadcasted_iota(jnp.int32, (SUB, ranks), 0)
    own_noise = jnp.zeros((SUB, ranks), F32)
    for t in range(0, width // LANES, SUB):
        part = noise_tiles[t : t + SUB, :]
        own_noise = jnp.where(
            tile == row + t, jnp.take_along_axis(part, lane, axis=1), own_noise
        )
    return own, jnp.sum(own_noise, axis=0, keepdims=True)


def pivot_covariance(dim, coords):
    ranks = coords.shape[1]
    across = coords.T
    total = jnp.zeros((ranks, ranks), F32)
    for d in range(dim):
        differ = across[:, d : d + 1] - coords[d : d + 1, :]
        total = total + differ * differ
    row = lax.broadcasted_iota(jnp.int32, (ranks, ranks), 0)
    col = lax.broadcasted_iota(jnp.int32, (ranks, ranks), 1)
    return jnp.exp(-0.5 * total) + jnp.where(row == col, coords[dim : dim + 1, :], 0.0)


def over_rows(x, i):
    return jnp.broadcast_to(x[i % SUB : i % SUB + 1], x.shape)


def over_lanes(x, j):
    return jnp.broadcast_to(x[:, j : j + 1], x.shape)


def gathered(rows):
    return [
        jnp.concatenate([rows[i][i % SUB : i % SUB + 1] for i in range(v, v + SUB)], axis=0)
        for v in range(0, len(rows), SUB)
    ]


def factor_block(rows, cols):
    size = SUB * len(rows)
    diag = over_rows(cols[0][0], 0)
    scales, factors, units = [], [], []
    for k in range(size):
        own = k // SUB
        r = lax.rsqrt(diag)
        if k + 1 < size:
            after = (k + 1) // SUB
            step = over_rows(cols[k][after], k + 1) * r
            diag = over_rows(cols[k + 1][after], k + 1) - step * step
        unit = over_rows(rows[own], k) * r
        col = [x * r if v >= own else None for v, x in enumerate(cols[k])]
        factor = {j: over_rows(col[j // SUB], j) for j in range(k + 1, size)}
        for j in range(k + 1, size):
            for v in range(j // SUB, len(rows)):
                cols[j][v] = cols[j][v] - col[v] * factor[j]
        for v in range((k + 1) // SUB, len(rows)):
            rows[v] = rows[v] - col[v] * unit
        scales.append(r)
        factors.append(factor)
        units.append(unit)
    done = gathered(units)
    for k in reversed(range(size)):
        units[k] = units[k] * scales[k]
        for i in range(k):
            units[i] = units[i] - factors[i][k] * units[k]
    return units, done


def wide_product(left, right, lo):
    ranks = left.shape[1]
    size = right.shape[0]
    h, m, l = split3(left)
    rh, rm, rl = (
        jnp.concatenate(
            [x for x in (jnp.zeros((lo, ranks), F32), y, jnp.zeros((ranks - lo - size, ranks), F32)) if x.shape[0]],
            axis=0,
        )
        for y in split3(right)
    )
    one = jnp.concatenate([rh, rm], axis=0).astype(BF16)
    two = jnp.concatenate([rh, rl], axis=0).astype(BF16)
    return (
        jnp.dot(jnp.concatenate([h, h], axis=1).astype(BF16), one, preferred_element_type=F32)
        + jnp.dot(jnp.concatenate([m, m], axis=1).astype(BF16), one, preferred_element_type=F32)
        + jnp.dot(jnp.concatenate([l, h], axis=1).astype(BF16), two, preferred_element_type=F32)
    )


def factor_rows(cov, between):
    ranks = cov.shape[0]
    count = 2
    size = count * SUB
    row = lax.broadcasted_iota(jnp.int32, (SUB, ranks), 0)
    col = lax.broadcasted_iota(jnp.int32, (SUB, ranks), 1)
    rows = [cov[i : i + SUB] for i in range(0, ranks, SUB)]
    done = []
    nothing = 0.0 * rows[0]
    late = None
    for lo in range(0, ranks, size):
        if late is not None:
            rows[count:] = late()
        inside = jnp.logical_and(col >= lo, col < lo + size)
        block, near, far = rows[0:count], rows[count : 2 * count], rows[2 * count :]
        lanes = range(lo, lo + size)
        cols = [
            [over_lanes(x, j) if lo + v * SUB + SUB > j else None for v, x in enumerate(block)]
            for j in lanes
        ]
        cols[0][0] = cols[0][0] + nothing
        cols[1][0] = cols[1][0] + nothing
        near_cols = [[over_lanes(x, j) for x in near] for j in lanes]
        block = [
            jnp.where(inside, jnp.where(row + (lo + v * SUB) == col, 1.0, 0.0), x)
            for v, x in enumerate(block)
        ]
        units, new = factor_block(block, cols)
        done += new
        rows = []
        for v, x in enumerate(near):
            terms = [near_cols[j][v] * units[j] for j in range(size)]
            while len(terms) > 1:
                terms = [p + q for p, q in zip(terms[::2], terms[1::2])]
            rows.append(jnp.where(inside, 0.0, x) - terms[0])

        def late(far=far, units=gathered(units), inside=inside, lo=lo):
            if not far:
                return []
            left = jnp.concatenate([jnp.where(inside, x, 0.0) for x in far], axis=0)
            out = wide_product(left, jnp.concatenate(units, axis=0), lo)
            return [
                jnp.where(inside, 0.0, x) - out[i * SUB : (i + 1) * SUB]
                for i, x in enumerate(far)
            ]

        rows += [None] * len(far)
        between(lo // size, done)
    return done


def pivot_side(dim, coords, centre):
    y = coords[0:dim, :] - centre
    yh, ym, yl = split3(LOG2E * y)
    nh, nm, nl = split3((-0.5 * LOG2E) * jnp.sum(y * y, axis=0, keepdims=True))
    ones = jnp.ones_like(nh)
    tail = [ones, ones, ones, nh, nm, nl, jnp.zeros((2 * dim - 6, y.shape[1]), F32)]
    return jnp.concatenate([yh, yh, ym, ym, yh, yl] + tail, axis=0).T.astype(BF16)


def point_side(dim, x):
    xh, xm, xl = split3(x)
    nh, nm, nl = split3((-0.5 * LOG2E) * jnp.sum(x * x, axis=0, keepdims=True))
    ones = jnp.ones_like(nh)
    tail = [nh, nm, nl, ones, ones, ones, jnp.zeros((2 * dim - 6, x.shape[1]), F32)]
    return jnp.concatenate([xh, xm, xh, xm, xl, xh] + tail, axis=0).astype(BF16)


def send(slots, k, device, send_sem, recv_sem):
    pltpu.make_async_remote_copy(
        src_ref=slots.at[0],
        dst_ref=slots.at[k],
        send_sem=send_sem,
        recv_sem=recv_sem,
        device_id=(device,),
        device_id_type=pl.DeviceIdType.MESH,
    ).start()


def all_of(slots, device, send_sem, recv_sem):
    rest = slots.at[pl.ds(1, slots.shape[0] - 1)]
    return pltpu.make_async_remote_copy(
        src_ref=rest,
        dst_ref=rest,
        send_sem=send_sem,
        recv_sem=recv_sem,
        device_id=(device,),
        device_id_type=pl.DeviceIdType.MESH,
    )


def total_of(slots):
    parts = [slots[k] for k in range(slots.shape[0])]
    while len(parts) > 1:
        parts = [a + b for a, b in zip(parts[::2], parts[1::2])] + (
            parts[-1:] if len(parts) % 2 else []
        )
    return parts[0]


def signal(sem, device):
    pl.semaphore_signal(
        sem, inc=1, device_id=(device,), device_id_type=pl.DeviceIdType.MESH
    )


def body_kernel(
    n, group, blocks, chunk,
    from_points, from_scales, from_noise, from_tiles, from_pivots,
    factor, residual, averages,
    points, scales, noise, noise_tiles, pivots,
    near_slots, far_slots, sum_slots, sides, pieces, explained,
    load_sem, send_sem, recv_sem, ready_sem, near_sent,
):
    dim, width = points.shape
    ranks = factor.shape[0]
    per_block = ranks // blocks
    me = lax.axis_index("rows")
    offset = me * width
    far_count = n // group
    low = lax.rem(me, group)
    level = (me - low) // group
    near = [me - low + lax.rem(low + k, group) for k in range(1, group)]
    far = [lax.rem(me + k * group, n) for k in range(1, far_count)]

    loads = [
        pltpu.make_async_copy(source, target, load_sem.at[i])
        for i, (source, target) in enumerate(
            [
                (from_points, points), (from_scales, scales), (from_noise, noise),
                (from_tiles, noise_tiles), (from_pivots, pivots),
            ]
        )
    ]
    for load in loads:
        load.start()
    barrier = pltpu.get_barrier_semaphore()
    for device in near:
        signal(barrier, device)
    for k in range(1, far_count):

        @pl.when(level + k < far_count)
        def _():
            signal(barrier, me + k * group)

    for load in loads:
        load.wait()
    scale = scale_column(dim, scales)
    pivot_row = jnp.concatenate([pivots[b : b + 1, :] for b in range(blocks)], axis=1)
    own, own_noise = gather_own(offset, pivot_row, points, noise_tiles)
    own = own / scale
    for d in range(dim):
        near_slots[0, d] = own[d : d + 1]
    near_slots[0, dim] = own_noise
    pl.semaphore_wait(barrier, group - 1 + level)
    for k, device in enumerate(near):
        send(near_slots, k + 1, device, near_sent.at[k], recv_sem.at[0])
    for k in range(1, far_count):

        @pl.when(level >= k)
        def _():
            signal(ready_sem, me - k * group)

    centre = jnp.sum(points[...], axis=1, keepdims=True) / (width * scale)
    base = jnp.zeros((SUB, LANES), F32)
    for t in range(0, width // LANES, SUB):
        base = base + (1.0 + noise_tiles[t : t + SUB, :])
    base = jnp.sum(jnp.sum(base, axis=1, keepdims=True), axis=0, keepdims=True)
    for c in range(width // chunk):
        at = slice(c * chunk, (c + 1) * chunk)
        sides[:, at] = point_side(dim, points[:, at] / scale - centre)

    all_of(near_slots, near[0], send_sem.at[0], recv_sem.at[0]).wait_recv()
    far_slots[0] = total_of(near_slots)

    @pl.when(level < far_count - 1)
    def _():
        pl.semaphore_wait(ready_sem, far_count - 1 - level)

    for k, device in enumerate(far):
        send(far_slots, k + 1, device, send_sem.at[1], recv_sem.at[1])
    all_of(far_slots, far[0], send_sem.at[1], recv_sem.at[1]).wait_recv()
    coords = total_of(far_slots)
    coords = jnp.concatenate([coords[d] for d in range(dim + 1)], axis=0)

    cov = pivot_covariance(dim, coords)
    side = pivot_side(dim, coords, centre)
    local_row = (pivot_row - offset).astype(F32)
    local_col = jnp.broadcast_to(local_row, (SUB, ranks)).T[:, 0:1].astype(jnp.int32)

    def cross_chunk(c):
        if c >= width // chunk:
            return
        at = slice(c * chunk, (c + 1) * chunk)
        cross = jnp.exp2(jnp.dot(side, sides[:, at], preferred_element_type=F32))
        ids = lax.broadcasted_iota(jnp.int32, (ranks, chunk), 1) + c * chunk
        cross = jnp.where(ids == local_col, 1.0 + noise[:, at], cross)
        high = cross.astype(BF16)
        pieces[0:ranks, at] = high
        pieces[ranks : 2 * ranks, at] = (cross - high.astype(F32)).astype(BF16)

    size = 2 * SUB
    rounds = ranks // size
    chunks = range(width // chunk)
    totals = [jnp.zeros((SUB, LANES), F32) for _ in range(blocks)]
    col = lax.broadcasted_iota(jnp.int32, (SUB, ranks), 1)
    row = lax.broadcasted_iota(jnp.int32, (SUB, ranks), 0)

    def lefts_of(done, top, bottom):
        part = [
            jnp.where(row + i * SUB >= col, done[i], 0.0)
            for i in range(top // SUB, bottom // SUB)
        ]
        high, mid, low = split3(jnp.concatenate(part, axis=0))
        tall = jnp.concatenate([low, mid, high], axis=0)
        return jnp.concatenate([tall, tall], axis=1).astype(BF16)

    def product(c, lefts, top, bottom):
        at = slice(c * chunk, (c + 1) * chunk)
        one = pieces[:, at]
        wide = jnp.dot(lefts, one, preferred_element_type=F32)
        rows = jnp.zeros((bottom - top, chunk), F32)
        for i in range(0, wide.shape[0], bottom - top):
            rows = rows + wide[i : i + bottom - top]
        factor[top:bottom, at] = rows
        square = rows * rows
        added = jnp.zeros((SUB, chunk), F32)
        for b in range(top // per_block, bottom // per_block):
            part = jnp.zeros((SUB, chunk), F32)
            for i in range(b * per_block - top, (b + 1) * per_block - top, SUB):
                part = part + square[i : i + SUB]
            added = added + part
            for j in range(0, chunk, LANES):
                totals[b] = totals[b] + part[:, j : j + LANES]
        return added

    def sent(k):
        return pltpu.make_async_remote_copy(
            src_ref=near_slots.at[0],
            dst_ref=near_slots.at[k + 1],
            send_sem=near_sent.at[k],
            recv_sem=recv_sem.at[0],
            device_id=(near[k],),
            device_id_type=pl.DeviceIdType.MESH,
        )

    early, middle = size * (rounds // 2), size * (rounds - 2)

    def share(r, first, last):
        each = -(-len(chunks) // (last - first))
        return chunks[(r - first) * each : (r - first + 1) * each] if first <= r < last else []

    def between(r, done):
        for c in share(r, 1, rounds // 2 + 1):
            cross_chunk(c)
        if rounds // 2 < r < rounds - 1:
            lefts = lefts_of(done, 0, early)
            for c in share(r, rounds // 2 + 1, rounds - 1):
                explained[:, c * chunk : (c + 1) * chunk] = product(c, lefts, 0, early)
        if r == rounds - 1:
            lefts = lefts_of(done, early, middle)
            for c in chunks:
                at = slice(c * chunk, (c + 1) * chunk)
                explained[:, at] = explained[:, at] + product(c, lefts, early, middle)
        if r < min(rounds - 1, len(near)):
            sent(r).wait_send()

    done = factor_rows(cov, between)
    lefts = lefts_of(done, middle, ranks)
    for c in chunks:
        at = slice(c * chunk, (c + 1) * chunk)
        added = explained[:, at] + product(c, lefts, middle, ranks)
        left = 1.0 + noise[:, at] - jnp.sum(added, axis=0, keepdims=True)
        residual[at] = left[0]

    total = jnp.concatenate([jnp.sum(x, axis=0, keepdims=True) for x in totals], axis=0)
    total = jnp.sum(total, axis=1, keepdims=True)
    row = lax.broadcasted_iota(jnp.int32, (blocks, LANES), 0)
    col = lax.broadcasted_iota(jnp.int32, (blocks, LANES), 1)
    done = jnp.sum(jnp.where(row <= col, total, 0.0), axis=0, keepdims=True)
    sum_slots[0] = base - done

    def send_sum(k, carry):
        send(sum_slots, k, lax.rem(me + k, n), send_sem.at[2], recv_sem.at[2])
        return carry

    lax.fori_loop(1, n, send_sum, 0)
    last = all_of(sum_slots, near[0], send_sem.at[2], recv_sem.at[2])
    for k in range(min(rounds - 1, len(near)), len(near)):
        sent(k).wait_send()
    all_of(far_slots, far[0], send_sem.at[1], recv_sem.at[1]).wait_send()
    last.wait_send()
    last.wait_recv()
    averages[...] = total_of(sum_slots)[0, 0:blocks] / (width * n)


def store_kernel(factor, residual, averages, to_factor, to_residual, to_averages, sem):
    copies = [
        pltpu.make_async_copy(source, target, sem.at[i])
        for i, (source, target) in enumerate(
            [(factor, to_factor), (residual, to_residual), (averages, to_averages)]
        )
    ]
    for copy in copies:
        copy.start()
    for copy in copies:
        copy.wait()


def body(n, points, scales, noise_var, pivots):
    dim, width = points.shape
    blocks, per_block = pivots.shape
    ranks = blocks * per_block
    chunk = 512
    group = 1
    while group * group < n:
        group *= 2
    vmem = pl.BlockSpec(memory_space=pltpu.VMEM)
    anywhere = pl.BlockSpec(memory_space=pl.ANY)
    factor, residual, averages = pl.pallas_call(
        functools.partial(body_kernel, n, group, blocks, chunk),
        name="whole",
        out_shape=(
            pltpu.VMEM((ranks, width), F32),
            pltpu.VMEM((width,), F32),
            pltpu.VMEM((blocks,), F32),
        ),
        in_specs=[anywhere] * 5,
        out_specs=(vmem, vmem, vmem),
        scratch_shapes=[
            pltpu.VMEM((dim, width), F32),
            pltpu.SMEM((dim,), F32),
            pltpu.VMEM((1, width), F32),
            pltpu.VMEM((width // LANES, LANES), F32),
            pltpu.VMEM(pivots.shape, jnp.int32),
            pltpu.VMEM((group, dim + 1, 1, ranks), F32),
            pltpu.VMEM((n // group, dim + 1, 1, ranks), F32),
            pltpu.VMEM((n, 1, LANES), F32),
            pltpu.VMEM((8 * dim, width), BF16),
            pltpu.VMEM((2 * ranks, width), BF16),
            pltpu.VMEM((SUB, width), F32),
            pltpu.SemaphoreType.DMA((5,)),
            pltpu.SemaphoreType.DMA((3,)),
            pltpu.SemaphoreType.DMA((3,)),
            pltpu.SemaphoreType.REGULAR,
            pltpu.SemaphoreType.DMA((group - 1,)),
        ],
        compiler_params=pltpu.CompilerParams(collective_id=0, has_side_effects=True),
    )(points, scales, noise_var.reshape(1, -1), noise_var.reshape(-1, LANES), pivots)
    return pl.pallas_call(
        store_kernel,
        name="store",
        out_shape=(
            jax.ShapeDtypeStruct((ranks, width), F32),
            jax.ShapeDtypeStruct((width,), F32),
            jax.ShapeDtypeStruct((blocks,), F32),
        ),
        in_specs=[vmem] * 3,
        out_specs=(anywhere,) * 3,
        scratch_shapes=[pltpu.SemaphoreType.DMA((3,))],
    )(*(pltpu.with_memory_space_constraint(x, pltpu.VMEM) for x in (factor, residual, averages)))


def solution(mesh):
    in_specs = (P(None, "rows"), P(), P("rows"), P())
    out_specs = (P(None, "rows"), P("rows"), P())
    return jax.shard_map(
        functools.partial(body, mesh.shape["rows"]),
        mesh=mesh, in_specs=in_specs, out_specs=out_specs, check_vma=False,
    )
```
